32 devices in a mesh: grp: 8 (over y, x, core), inner: 4 (over z).
Axes of the slice: x: 2, y: 2, z: 4, core: 2. Of those that a mesh axis runs over, the one named last changes fastest.
Arguments:
- amplitudes: bfloat16 [16, 8, 12288], P('grp', None, 'inner'), may hold values from -6 to 6
- factors: bfloat16 [16, 2000, 12288], P('grp', 'inner'), may hold values from -0.125 to 0.125
- atom_charges: bfloat16 [16, 64, 12288], P('grp', None, 'inner'), may hold values from -0.0068359375 to 0.0068359375
- eps_occ: float32 [16, 48], P('grp'), may hold values from -1.2 to -0.3
- eps_vir: float32 [16, 256], P('grp'), may hold values from 0.1 to 1.5
- occ_count: int32 [16], P('grp'), may hold values from 24 to 48
- vir_count: int32 [16], P('grp'), may hold values from 128 to 256
- atom_list: int32 [1024], P('grp'), may hold values from 0 to 1023, each once
- positions: float32 [3, 1024], replicated, may hold values from 0 to 12
Outputs:
- refined: float32 [16, 8, 12288], P('grp', None, 'inner')
- hamiltonian: float32 [128, 8, 16], P('grp', None, 'inner')
The draws below stay inside these ranges and needn't reach their ends.
Inputs may be any that keep to these rules, and one draw needn't show every extreme that they name: `atom_list`: every atom index appears exactly once.
All inputs are finite; a program needn't handle non-finite values.
Results may differ from the reference program's by a relative error of at most 0.022.
Values may be sent and summed in bfloat16 or wider, within the bound.
No kernel may reach another device: no remote copies, remote signals or barrier semaphores. Data moves between devices by JAX's collectives and lax.ppermute only.
A program may use at most 64 MiB of HBM per device.

```python
import functools
import jax
import jax.numpy as jnp
from jax import lax

NOCC = 48
NVIR = 256
NAUX = 2000
STATES = 8
ATOMS = 64
OV = 12288
CHROMOPHORES = 16
ALL_ATOMS = 1024
GSTATES = 16
NSTATE = 128
N_GRP = 8
N_INNER = 4


def place_ends(drawn, stream_key, low, largest):
    longest = drawn.shape.index(max(drawn.shape))
    spots = []
    for shift in (0, 1):
        where = [jax.random.randint(jax.random.fold_in(stream_key, axis), (), 0, length) for axis, length in enumerate(drawn.shape)]
        where[longest] = (where[longest] + shift) % drawn.shape[longest]
        spots.append(tuple(where))
    return drawn.at[spots[0]].set(low).at[spots[1]].set(largest)


def block_levels(rng, dims, shards, smallest, largest):
    gain, own = 1.0, jax.random.fold_in(rng, 6)
    for position, parts in shards:
        draws = jnp.exp(jax.random.uniform(jax.random.fold_in(own, position), (parts,), jnp.float32, smallest / len(shards), largest / len(shards)))
        gain = gain * jnp.repeat(draws, dims[position] // parts).reshape([-1 if axis == position else 1 for axis in range(len(dims))])
    return gain


def bell_draw(stream_key, extent, width, most, cuts=(), held_as=jnp.bfloat16):
    entries = width * jax.random.normal(stream_key, extent, jnp.float32)
    if cuts:
        entries = entries * block_levels(stream_key, extent, cuts, -0.22, 0.18)
    return jnp.clip(entries, -most, most).astype(held_as)


def setup_inputs(seed: int = 0) -> dict:
    arg_keys = jax.random.split(jax.random.key(seed), 10)
    amplitudes = bell_draw(arg_keys[0], (CHROMOPHORES, STATES, OV), 1.0, 6.0, ((0, 8), (2, 4)))
    factors = bell_draw(arg_keys[1], (CHROMOPHORES, NAUX, OV), NAUX ** -0.5, 0.125, ((0, 8), (1, 4)))
    atom_charges = bell_draw(arg_keys[2], (CHROMOPHORES, ATOMS, OV), (OV * ATOMS) ** -0.5, 0.0068359375, ((0, 8), (2, 4)))
    eps_occ = jnp.clip(-1.2 + 0.90000004 * jax.random.uniform(arg_keys[3], (CHROMOPHORES, NOCC), jnp.float32) ** block_levels(arg_keys[3], (CHROMOPHORES, NOCC), ((0, 8),), -0.2, 0.2), -1.2, -0.3)
    eps_vir = jnp.clip(0.1 + 1.4 * jax.random.uniform(arg_keys[4], (CHROMOPHORES, NVIR), jnp.float32) ** block_levels(arg_keys[4], (CHROMOPHORES, NVIR), ((0, 8),), -0.2, 0.2), 0.1, 1.5)
    occ_count = place_ends(jax.random.randint(arg_keys[5], (CHROMOPHORES,), NOCC // 2, NOCC + 1), jax.random.fold_in(arg_keys[5], 1), NOCC // 2, NOCC).astype(jnp.int32)
    vir_count = place_ends(jax.random.randint(arg_keys[6], (CHROMOPHORES,), NVIR // 2, NVIR + 1), jax.random.fold_in(arg_keys[6], 1), NVIR // 2, NVIR).astype(jnp.int32)
    atom_list = jax.random.permutation(arg_keys[7], ALL_ATOMS).astype(jnp.int32)
    positions = jnp.clip(jax.random.uniform(arg_keys[8], (3, ALL_ATOMS), jnp.float32, 0.0, 12.0), 0.0, 12.0)
    return {"amplitudes": amplitudes, "factors": factors, "atom_charges": atom_charges, "eps_occ": eps_occ, "eps_vir": eps_vir, "occ_count": occ_count, "vir_count": vir_count, "atom_list": atom_list, "positions": positions}


epsilon = 1e-06

def monomer(packed):
    factor, current, charge_map, occ_energy, vir_energy, occ_limit, vir_limit = packed
    pair_index = jnp.arange(OV, dtype=jnp.int32)
    occ_of = pair_index // NVIR
    vir_of = pair_index % NVIR
    active = ((occ_of < occ_limit) & (vir_of < vir_limit)).astype(jnp.float32)
    gap = vir_energy[vir_of] - occ_energy[occ_of]
    masked = current * active.astype(jnp.bfloat16)[None, :]
    fitted = jnp.dot(masked, factor.T, preferred_element_type=jnp.float32)
    fitted_low = fitted.astype(jnp.bfloat16)
    block_aux = NAUX // N_INNER
    fitted_blocks = fitted_low.astype(jnp.float32).reshape(STATES, N_INNER, block_aux)
    factor_blocks = factor.astype(jnp.float32).reshape(N_INNER, block_aux, OV)
    partial_value = 2.0 * jnp.einsum('sja,jao->jso', fitted_blocks, factor_blocks)
    coulomb = lax.optimization_barrier(jnp.sum(partial_value.astype(jnp.bfloat16).astype(jnp.float32), axis=0))
    start = masked.astype(jnp.float32)
    image = gap[None, :] * start + coulomb * active[None, :]
    energies = lax.optimization_barrier(jnp.sum(start * image, axis=1)) / (lax.optimization_barrier(jnp.sum(start * start, axis=1)) + epsilon)
    refined = active[None, :] * (start - (image - energies[:, None] * start) / gap[None, :])
    charges = jnp.dot(refined.astype(jnp.bfloat16), charge_map.T, preferred_element_type=jnp.float32)
    return (refined, charges, energies)

def coupling_rows(packed, xyz_all, charges_all):
    own_xyz, own_charges, own_energy, which = packed
    offset = own_xyz[:, :, None, None] - jnp.transpose(xyz_all, (1, 0, 2))[:, None, :, :]
    kernel = 1.0 / jnp.sqrt(lax.optimization_barrier(jnp.sum(offset * offset, axis=0)) + 1.0)
    block = jnp.einsum('sa,adb,dtb->sdt', own_charges, kernel, charges_all, precision=lax.Precision.HIGHEST)
    same = (jnp.arange(CHROMOPHORES, dtype=jnp.int32) == which)[None, :, None]
    diagonal = jnp.eye(STATES, dtype=jnp.float32)[:, None, :] * own_energy[:, None, None]
    return jnp.where(same, diagonal, block)

def reference(amplitudes, factors, atom_charges, eps_occ, eps_vir, occ_count, vir_count, atom_list, positions):
    refined, charges, energies = lax.map(monomer, (factors, amplitudes, atom_charges, eps_occ, eps_vir, occ_count, vir_count))
    coords = jnp.take(positions, atom_list, axis=1).reshape(3, CHROMOPHORES, ATOMS).transpose(1, 0, 2)
    which = jnp.arange(CHROMOPHORES, dtype=jnp.int32)
    blocks = lax.map(functools.partial(coupling_rows, xyz_all=coords, charges_all=charges), (coords, charges, energies, which))
    return (refined, blocks.reshape(NSTATE, N_GRP, GSTATES))
```

```python
import functools

import jax
import jax.numpy as jnp
from jax import lax
from jax.experimental import pallas as pl
from jax.experimental.pallas import tpu as pltpu
from jax.sharding import PartitionSpec as P

epsilon = 1e-06
LANES = 128
CHUNK = 256
NT = (((1,), (1,)), ((), ()))


SMEM = pl.BlockSpec(memory_space=pltpu.SMEM)
VMEM = pl.BlockSpec(memory_space=pltpu.VMEM)
PARAMS = pltpu.CompilerParams(vmem_limit_bytes=16 * 2**20)
HBM = pl.BlockSpec(memory_space=pltpu.HBM)


def masked_chunk(amp, occ_count, vir_count, occ):
    lim = jnp.where(occ < occ_count, vir_count, 0)
    on = lax.broadcasted_iota(jnp.int32, amp.shape, 1) < lim
    return jnp.where(on, amp.astype(jnp.float32), 0.0), on


def first_kernel(
    pos_ref, count_ref, occ_ref, vir_ref, amp_ref, atom_ref, xyz_ref, factor_hbm,
    factor_ref, fit_ref, sums_ref, own_xyz_ref, mask_ref, sems, *, chunks,
):
    rows, pairs = amp_ref.shape
    monomers, nvir = vir_ref.shape
    states = rows // monomers
    tiles = pairs // LANES
    pos = pos_ref[0]

    for k, (start, size) in enumerate(chunks):

        def issue(q, carry, k=k):
            pltpu.make_async_copy(
                factor_hbm.at[q], factor_ref.at[:, pl.ds(q * monomers, monomers)], sems.at[k]
            ).start()
            return carry

        lax.fori_loop(start, start + size, issue, 0)
    for c in range(monomers):
        top = jnp.zeros((states, nvir), jnp.float32)
        square = jnp.zeros((states, nvir), jnp.float32)
        span = slice(c * states, (c + 1) * states)
        for b in range(pairs // nvir):
            occ = pos * (pairs // nvir) + b
            cut = slice(b * nvir, (b + 1) * nvir)
            value, _ = masked_chunk(amp_ref[span, cut], count_ref[0, c], count_ref[1, c], occ)
            mask_ref[span, cut] = value.astype(jnp.bfloat16)
            gap = vir_ref[c : c + 1, :] - occ_ref[c, occ]
            value2 = value * value
            square = square + value2
            top = top + gap * value2
        total = jnp.sum(top, axis=1, keepdims=True)
        norm = jnp.sum(square, axis=1, keepdims=True)
        lane = lax.broadcasted_iota(jnp.int32, (states, LANES), 1)
        sums_ref[span, :] = jnp.where(lane == 0, total, jnp.where(lane == 1, norm, 0.0))
    table = xyz_ref.shape[1]
    hot = lax.broadcasted_iota(jnp.int32, (table, atom_ref.shape[1]), 0) == atom_ref[...]
    own_xyz_ref[...] = jnp.dot(
        xyz_ref[...], hot.astype(jnp.float32), precision=lax.Precision.HIGHEST,
        preferred_element_type=jnp.float32,
    )
    masked = mask_ref[...]
    for k, (start, size) in enumerate(chunks):
        whole = factor_hbm.at[start : start + size]
        pltpu.make_async_copy(whole, whole, sems.at[k]).wait()
        span = slice(start * monomers, (start + size) * monomers)
        block = jnp.concatenate([factor_ref[pos * tiles + t, span] for t in range(tiles)], axis=1)
        fit_ref[:, span] = lax.dot_general(masked, block, NT, preferred_element_type=jnp.float32)


def second_kernel(pos_ref, count_ref, *refs, inner, monomers, nvir):
    amps = refs[: inner - 1]
    factor_ref, fit_ref, sums_ref = refs[inner - 1 : inner + 2]
    outs = refs[inner + 2 : 2 * inner + 2]
    mask_ref = refs[-1]
    rows, pairs = amps[0].shape
    states = rows // monomers
    tiles = pairs // LANES
    pos = pos_ref[0]

    def where(r):
        return lax.rem(pos + inner - r, inner)

    for r in range(1, inner):
        for c in range(monomers):
            span = slice(c * states, (c + 1) * states)
            for b in range(pairs // nvir):
                cut = slice(b * nvir, (b + 1) * nvir)
                value, _ = masked_chunk(
                    amps[r - 1][span, cut], count_ref[0, c], count_ref[1, c],
                    where(r) * (pairs // nvir) + b,
                )
                mask_ref[r - 1, span, cut] = value.astype(jnp.bfloat16)

    def add(r, fit):
        at = where(r) * tiles
        block = jnp.concatenate([factor_ref[at + t] for t in range(tiles)], axis=1)
        return fit + lax.dot_general(
            mask_ref[r - 1], block, NT, preferred_element_type=jnp.float32
        )

    fit = lax.fori_loop(1, inner, add, fit_ref[...])
    row = lax.broadcasted_iota(jnp.int32, fit.shape, 0) // states
    column = lax.broadcasted_iota(jnp.int32, fit.shape, 1) % monomers
    fit = jnp.where(row == column, fit, 0.0)
    low = fit.astype(jnp.bfloat16)
    extra = 2.0 * jnp.sum(low.astype(jnp.float32) * fit, axis=1, keepdims=True)
    lane = lax.broadcasted_iota(jnp.int32, (rows, LANES), 1)
    total = sums_ref[...] + jnp.where(lane == 0, extra, 0.0)
    high = total.astype(jnp.bfloat16).astype(jnp.float32)
    rest = total - high
    middle = rest.astype(jnp.bfloat16).astype(jnp.float32)
    tail = rest - middle
    pieces = (high + pltpu.roll(middle, 2, 1) + pltpu.roll(tail, 4, 1)).astype(jnp.bfloat16)
    group = next(g for g in (8, 6, 4, 2, 1) if tiles % g == 0)
    for k in range(inner):
        r = (k + 1) % inner
        at = where(r) * tiles
        out = outs[r]

        def step(i, carry, at=at, out=out):
            block = jnp.concatenate([factor_ref[at + i * group + t] for t in range(group)], axis=1)
            part = jnp.dot(low, block, preferred_element_type=jnp.float32)
            cut = pl.ds(pl.multiple_of(i * (group * LANES), LANES), group * LANES)
            out[:, cut] = (2.0 * part).astype(jnp.bfloat16)
            return carry

        lax.fori_loop(0, tiles // group, step, 0)
        out[:, pairs:] = pieces


def third_kernel(pos_ref, count_ref, occ_ref, vir_ref, amp_ref, map_ref, *refs, inner):
    parts = refs[:inner]
    refined_ref, charge_ref, low_ref = refs[inner:]
    rows, pairs = amp_ref.shape
    monomers, atoms = map_ref.shape[:2]
    states = rows // monomers
    nvir = vir_ref.shape[1]
    pos = pos_ref[0]
    tail = sum(p[:, pairs:].astype(jnp.float32) for p in parts)
    lane = lax.broadcasted_iota(jnp.int32, tail.shape, 1)
    top = jnp.sum(jnp.where((lane < 6) & (lane % 2 == 0), tail, 0.0), axis=1, keepdims=True)
    norm = jnp.sum(jnp.where((lane < 6) & (lane % 2 == 1), tail, 0.0), axis=1, keepdims=True)
    energies = top / (norm + epsilon)
    for c in range(monomers):
        span = slice(c * states, (c + 1) * states)
        energy = energies[span]
        for b in range(pairs // nvir):
            occ = pos * (pairs // nvir) + b
            cut = slice(b * nvir, (b + 1) * nvir)
            value, on = masked_chunk(amp_ref[span, cut], count_ref[0, c], count_ref[1, c], occ)
            coulomb = sum(p[span, cut].astype(jnp.float32) for p in parts)
            inverse = 1.0 / (vir_ref[c : c + 1, :] - occ_ref[c, occ])
            refined = jnp.where(on, (energy * value - coulomb) * inverse, 0.0)
            refined_ref[span, cut] = refined
            low_ref[c, :, cut] = refined.astype(jnp.bfloat16)
        charge_ref[span, :atoms] = lax.dot_general(
            low_ref[c], map_ref[c], NT, preferred_element_type=jnp.float32
        )
        charge_ref[span, atoms:] = jnp.broadcast_to(energy, (states, LANES - atoms))


def fourth_kernel(pos_ref, xyz_ref, *refs, inner, share, states):
    parts = refs[:inner]
    charge_ref, send_ref = refs[inner:]
    atoms = xyz_ref.shape[1] * states // charge_ref.shape[0]
    pos = pos_ref[0]
    lane = lax.broadcasted_iota(jnp.int32, charge_ref.shape, 1)
    total = parts[0][...]
    for p in parts[1:]:
        total = total + jnp.where(lane < atoms, p[...], 0.0)
    charge_ref[...] = total
    send_ref[...] = jnp.zeros(send_ref.shape, jnp.float32)
    send_ref[0:share, :] = charge_ref[pl.ds(pos * share, share), :]
    which = (pos * share) // states
    xyz = xyz_ref[...]
    chosen = xyz[:, 0:atoms]
    for c in range(1, charge_ref.shape[0] // states):
        chosen = jnp.where(which == c, xyz[:, c * atoms : (c + 1) * atoms], chosen)
    send_ref[share : share + 3, :atoms] = chosen


def fifth_kernel(pos_ref, charge_ref, xyz_ref, *refs, groups, share, states, atoms):
    parts = refs[:groups]
    out_ref, columns_ref, wide_ref = refs[groups:]
    rows = charge_ref.shape[0]
    monomers = rows // states
    pos, group = pos_ref[0], pos_ref[1]
    columns_ref[...] = jnp.transpose(
        jnp.concatenate([xyz_ref[...], jnp.zeros((5, xyz_ref.shape[1]), jnp.float32)], axis=0)
    )
    for k in range(groups):
        wide_ref[:, k * atoms : (k + 1) * atoms] = parts[k][:, :atoms]
    weights = []
    for c in range(monomers):
        square = None
        for axis in range(3):
            diff = (
                columns_ref[c * atoms : (c + 1) * atoms, axis : axis + 1]
                - wide_ref[share + axis : share + axis + 1, :]
            )
            square = diff * diff if square is None else square + diff * diff
        inverse = 1.0 / jnp.sqrt(square + 1.0)
        weights.append(
            jnp.dot(
                charge_ref[c * states : (c + 1) * states, :atoms], inverse,
                precision=lax.Precision.HIGHEST, preferred_element_type=jnp.float32,
            )
        )
    weight = jnp.concatenate(weights, axis=0)
    row = lax.broadcasted_iota(jnp.int32, (share, rows), 1)
    column = pos * share + lax.broadcasted_iota(jnp.int32, (share, rows), 0)
    energy = jnp.transpose(charge_ref[...])[atoms : atoms + 1, :]
    for k in range(groups):
        source = lax.rem(group + groups - k, groups)
        block = lax.dot_general(
            parts[k][0:share, :atoms], weight[:, k * atoms : (k + 1) * atoms], NT,
            precision=lax.Precision.HIGHEST, preferred_element_type=jnp.float32,
        )
        if k == 0:
            same = row // states == column // states
            block = jnp.where(same, jnp.where(row == column, energy, 0.0), block)
        out_ref[source] = block


def local(
    amplitudes, factors, atom_charges, eps_occ, eps_vir, occ_count, vir_count, atom_list, positions
):
    monomers, states, pairs = amplitudes.shape
    aux = factors.shape[1]
    atoms = atom_charges.shape[1]
    nvir = eps_vir.shape[1]
    inner, groups = lax.axis_size("inner"), lax.axis_size("grp")
    rows = monomers * states
    share = rows // inner
    assert pairs % nvir == 0 and states % share == 0 and atoms < LANES and share + 3 <= 8
    f32, bf16 = jnp.float32, jnp.bfloat16
    where = jnp.stack([lax.axis_index("inner"), lax.axis_index("grp")]).astype(jnp.int32)
    counts = jnp.stack([occ_count, vir_count])

    def shift(value, axis, size, k):
        return lax.ppermute(value, axis, [(i, (i + k) % size) for i in range(size)])

    amplitudes = amplitudes.reshape(rows, pairs)
    amps = [shift(amplitudes, "inner", inner, r) for r in range(1, inner)]
    tiles = factors.shape[2] // LANES
    stored = factors.transpose(1, 0, 2).reshape(aux, monomers, tiles, LANES).transpose(0, 2, 1, 3)
    chunks = [(q, min(CHUNK, aux - q)) for q in range(0, aux, CHUNK)]
    factor_here, fit, sums, own_xyz = pl.pallas_call(
        functools.partial(first_kernel, chunks=chunks),
        in_specs=[SMEM, SMEM, SMEM, VMEM, VMEM, VMEM, VMEM, HBM],
        out_specs=[VMEM] * 4,
        out_shape=[
            pltpu.VMEM((tiles, aux * monomers, LANES), bf16),
            jax.ShapeDtypeStruct((rows, aux * monomers), f32),
            jax.ShapeDtypeStruct((rows, LANES), f32),
            jax.ShapeDtypeStruct((3, monomers * atoms), f32),
        ],
        scratch_shapes=[
            pltpu.VMEM((rows, pairs), bf16),
            pltpu.SemaphoreType.DMA((len(chunks),)),
        ],
        compiler_params=PARAMS,
        name="first",
    )(where, counts, eps_occ, eps_vir, amplitudes, atom_list[None, :], positions, stored)
    factor_here = pltpu.with_memory_space_constraint(factor_here, pltpu.VMEM)
    parts = pl.pallas_call(
        functools.partial(second_kernel, inner=inner, monomers=monomers, nvir=nvir),
        in_specs=[SMEM, SMEM] + [VMEM] * (inner + 2),
        out_specs=[VMEM] * inner,
        out_shape=[jax.ShapeDtypeStruct((rows, pairs + LANES), bf16)] * inner,
        scratch_shapes=[pltpu.VMEM((inner - 1, rows, pairs), bf16)],
        compiler_params=PARAMS,
        name="second",
    )(where, counts, *amps, factor_here, fit, sums)
    got = [parts[0]] + [shift(parts[r], "inner", inner, -r) for r in range(1, inner)]
    refined, charge = pl.pallas_call(
        functools.partial(third_kernel, inner=inner),
        in_specs=[SMEM, SMEM, SMEM] + [VMEM] * (inner + 3),
        out_specs=[VMEM] * 2,
        out_shape=[
            jax.ShapeDtypeStruct((rows, pairs), f32),
            jax.ShapeDtypeStruct((rows, LANES), f32),
        ],
        scratch_shapes=[pltpu.VMEM((monomers, states, pairs), bf16)],
        compiler_params=PARAMS,
        name="third",
    )(where, counts, eps_occ, eps_vir, amplitudes, atom_charges, *got)
    charges = [charge] + [shift(charge, "inner", inner, r) for r in range(1, inner)]
    charge, send = pl.pallas_call(
        functools.partial(fourth_kernel, inner=inner, share=share, states=states),
        in_specs=[SMEM] + [VMEM] * (inner + 1),
        out_specs=[VMEM] * 2,
        out_shape=[
            jax.ShapeDtypeStruct((rows, LANES), f32),
            jax.ShapeDtypeStruct((8, LANES), f32),
        ],
        compiler_params=PARAMS,
        name="fourth",
    )(where, own_xyz, *charges)
    sends = [send] + [shift(send, "grp", groups, k) for k in range(1, groups)]
    block = pl.pallas_call(
        functools.partial(fifth_kernel, groups=groups, share=share, states=states, atoms=atoms),
        in_specs=[SMEM] + [VMEM] * (groups + 2),
        out_specs=VMEM,
        out_shape=jax.ShapeDtypeStruct((groups, share, rows), f32),
        scratch_shapes=[
            pltpu.VMEM((monomers * atoms, 8), f32),
            pltpu.VMEM((8, groups * atoms), f32),
        ],
        compiler_params=PARAMS,
        name="fifth",
    )(where, charge, own_xyz, *sends)
    return refined.reshape(monomers, states, pairs), block.transpose(2, 0, 1)


def solution(mesh):
    in_specs = (
        P("grp", None, "inner"),
        P("grp", "inner", None),
        P("grp", None, "inner"),
        P("grp", None),
        P("grp", None),
        P("grp"),
        P("grp"),
        P("grp"),
        P(),
    )
    out_specs = (P("grp", None, "inner"), P("grp", None, "inner"))
    return jax.shard_map(local, mesh=mesh, in_specs=in_specs, out_specs=out_specs, check_vma=False)
```

```python
import functools

import jax
import jax.numpy as jnp
from jax import lax
from jax.experimental import pallas as pl
from jax.experimental.pallas import tpu as pltpu
from jax.sharding import PartitionSpec as P

epsilon = 1e-06
LANES = 128
CHUNK = 256
TAIL = 64
STEP = 2
COST = 10**8
NT = (((1,), (1,)), ((), ()))


VMEM = pl.BlockSpec(memory_space=pltpu.VMEM)
PARAMS = pltpu.CompilerParams(vmem_limit_bytes=16 * 2**20)
HBM = pl.BlockSpec(memory_space=pltpu.HBM)


def fetch(pairs, sem):
    copies = [pltpu.make_async_copy(src, dst, sem.at[k]) for k, (src, dst) in enumerate(pairs)]
    for copy in copies:
        copy.start()
    return copies


def first_kernel(
    *refs, chunks,
):
    sources, factor_hbm = refs[:7], refs[7]
    factor_ref, fit_ref, sums_ref, own_xyz_ref, mask_ref, active_ref, inverse_ref = refs[8:15]
    occs_ref, virs_ref, occ_ref, vir_ref, amp_ref, atom_ref, xyz_ref = refs[15:22]
    sems, small = refs[22:]
    copies = fetch(list(zip(sources, refs[15:22])), small)
    rows, pairs = amp_ref.shape
    monomers, nvir = vir_ref.shape
    states = rows // monomers
    tiles = pairs // LANES
    pos = lax.axis_index("inner")

    for k, (start, size) in enumerate(chunks):

        def issue(q, carry, k=k):
            pltpu.make_async_copy(
                factor_hbm.at[q], factor_ref.at[:, pl.ds(q * monomers, monomers)], sems.at[k]
            ).start()
            return carry

        lax.fori_loop(start, start + size, issue, 0)
    for copy in copies:
        copy.wait()
    column = lax.broadcasted_iota(jnp.int32, (1, nvir), 1)
    for c in range(monomers):
        for occ in range(active_ref.shape[1] // nvir):
            limit = jnp.where(occ < occs_ref[c], virs_ref[c], 0)
            active_ref[c : c + 1, occ * nvir : (occ + 1) * nvir] = (column < limit).astype(jnp.float32)
    for c in range(monomers):
        top = jnp.zeros((states, nvir), jnp.float32)
        square = jnp.zeros((states, nvir), jnp.float32)
        span = slice(c * states, (c + 1) * states)
        for b in range(pairs // nvir):
            occ = pos * (pairs // nvir) + b
            cut = slice(b * nvir, (b + 1) * nvir)
            active = active_ref[c : c + 1, pl.ds(pl.multiple_of(occ * nvir, LANES), nvir)]
            value = amp_ref[span, cut].astype(jnp.float32) * active
            mask_ref[span, cut] = value.astype(jnp.bfloat16)
            gap = vir_ref[c : c + 1, :] - occ_ref[c, occ]
            inverse_ref[c : c + 1, cut] = active / gap
            value2 = value * value
            square = square + value2
            top = top + gap * value2
        total = jnp.sum(top, axis=1, keepdims=True)
        norm = jnp.sum(square, axis=1, keepdims=True)
        lane = lax.broadcasted_iota(jnp.int32, (states, LANES), 1)
        sums_ref[span, :] = jnp.where(lane == 0, total, jnp.where(lane == 1, norm, 0.0))
    table = xyz_ref.shape[1]
    hot = lax.broadcasted_iota(jnp.int32, (table, atom_ref.shape[1]), 0) == atom_ref[...]
    own_xyz_ref[...] = jnp.dot(
        xyz_ref[...], hot.astype(jnp.float32), precision=lax.Precision.HIGHEST,
        preferred_element_type=jnp.float32,
    )
    masked = mask_ref[...]
    for k, (start, size) in enumerate(chunks):
        whole = factor_hbm.at[start : start + size]
        pltpu.make_async_copy(whole, whole, sems.at[k]).wait()
        span = slice(start * monomers, (start + size) * monomers)
        block = jnp.concatenate([factor_ref[pos * tiles + t, span] for t in range(tiles)], axis=1)
        if size < CHUNK // 2:
            streamed = lax.dot_general(block, masked, NT, preferred_element_type=jnp.float32)
            fit_ref[:, span] = jnp.transpose(streamed)
        else:
            fit_ref[:, span] = lax.dot_general(
                masked, block, NT, preferred_element_type=jnp.float32
            )


def block_of(low, pieces, factor_ref, at, out, most):
    tiles = (out.shape[1] - LANES) // LANES
    group = next(g for g in range(most, 0, -1) if tiles % g == 0)

    def step(i, carry):
        block = jnp.concatenate([factor_ref[at + i * group + t] for t in range(group)], axis=1)
        part = jnp.dot(low, block, preferred_element_type=jnp.float32)
        cut = pl.ds(pl.multiple_of(i * (group * LANES), LANES), group * LANES)
        out[:, cut] = (2.0 * part).astype(jnp.bfloat16)
        return carry

    lax.fori_loop(0, tiles // group, step, 0)
    out[:, tiles * LANES :] = pieces


def second_kernel(*refs, inner, monomers):
    amps = refs[: inner - 1]
    factor_ref, fit_ref, sums_ref, active_ref = refs[inner - 1 : inner + 3]
    low_ref, pieces_ref, mask_ref = refs[inner + 3 :]
    rows, pairs = amps[0].shape
    states = rows // monomers
    tiles = pairs // LANES
    pos = lax.axis_index("inner")
    for r in range(1, inner):
        for c in range(monomers):
            span = slice(c * states, (c + 1) * states)
            at = pl.multiple_of((pos ^ r) * pairs, LANES)
            value = amps[r - 1][span, :].astype(jnp.float32) * active_ref[c : c + 1, pl.ds(at, pairs)]
            mask_ref[r - 1, span, :] = value.astype(jnp.bfloat16)

    wide = fit_ref.shape[1]
    still = min(wide, -(-wide // 512) * 256)
    step = next(g for g in (STEP, 4, 2, 1) if tiles % g == 0)
    left = jnp.zeros((rows, still), jnp.float32)
    right = 0.0
    for r in range(1, inner):
        at = (pos ^ r) * tiles
        for t in range(0, tiles, step):
            value = mask_ref[r - 1, :, t * LANES : (t + step) * LANES]
            block = jnp.concatenate([factor_ref[at + t + u, :still] for u in range(step)], axis=1)
            left = left + lax.dot_general(value, block, NT, preferred_element_type=jnp.float32)
            if still < wide:
                block = jnp.concatenate([factor_ref[at + t + u, still:] for u in range(step)], axis=1)
                right = right + lax.dot_general(
                    block, value, NT, preferred_element_type=jnp.float32
                )
    if still < wide:
        left = jnp.concatenate([left, jnp.transpose(right)], axis=1)
    fit = fit_ref[...] + left
    row = lax.broadcasted_iota(jnp.int32, fit.shape, 0) // states
    column = lax.broadcasted_iota(jnp.int32, fit.shape, 1) % monomers
    fit = jnp.where(row == column, fit, 0.0)
    low = fit.astype(jnp.bfloat16)
    extra = 2.0 * jnp.sum(low.astype(jnp.float32) * fit, axis=1, keepdims=True)
    lane = lax.broadcasted_iota(jnp.int32, (rows, LANES), 1)
    total = sums_ref[...] + jnp.where(lane == 0, extra, 0.0)
    high = total.astype(jnp.bfloat16).astype(jnp.float32)
    rest = total - high
    middle = rest.astype(jnp.bfloat16).astype(jnp.float32)
    tail = rest - middle
    pieces = (high + pltpu.roll(middle, 2, 1) + pltpu.roll(tail, 4, 1)).astype(jnp.bfloat16)
    low_ref[...] = low
    pieces_ref[...] = pieces


def part_kernel(low_ref, pieces_ref, factor_ref, out_ref, *, r):
    tiles = (out_ref.shape[1] - LANES) // LANES
    block_of(low_ref[...], pieces_ref[...], factor_ref, (lax.axis_index("inner") ^ r) * tiles, out_ref, 24)


def third_kernel(masked_ref, inverse_ref, map_ref, *refs, inner):
    parts, xyz_ref = refs[:inner], refs[inner]
    refined_ref, send_ref, energy_ref, charge_ref, low_ref = refs[inner + 1 :]
    rows, pairs = masked_ref.shape
    monomers, atoms = map_ref.shape[:2]
    states = rows // monomers
    tail = sum(p[:, pairs:].astype(jnp.float32) for p in parts)
    lane = lax.broadcasted_iota(jnp.int32, tail.shape, 1)
    top = jnp.sum(jnp.where((lane < 6) & (lane % 2 == 0), tail, 0.0), axis=1, keepdims=True)
    norm = jnp.sum(jnp.where((lane < 6) & (lane % 2 == 1), tail, 0.0), axis=1, keepdims=True)
    energies = top / (norm + epsilon)
    energy_ref[...] = jnp.transpose(jnp.broadcast_to(energies, (rows, LANES)))[0:8, :]
    charge_ref[...] = jnp.zeros(charge_ref.shape, jnp.float32)
    for c in range(monomers):
        span = slice(c * states, (c + 1) * states)
        energy = energies[span]
        coulomb = sum(p[span, :pairs].astype(jnp.float32) for p in parts)
        value = masked_ref[span, :].astype(jnp.float32)
        refined = (energy * value - coulomb) * inverse_ref[c : c + 1, :]
        refined_ref[span, :] = refined
        low_ref[c] = refined.astype(jnp.bfloat16)
        charge_ref[span, :atoms] = lax.dot_general(
            low_ref[c], map_ref[c], NT, preferred_element_type=jnp.float32
        )
    which = lax.rem(lax.axis_index("inner"), monomers)
    xyz = xyz_ref[:, :atoms]
    for c in range(1, monomers):
        xyz = jnp.where(which == c, xyz_ref[:, c * atoms : (c + 1) * atoms], xyz)
    for piece in range(3):
        part = xyz.astype(jnp.bfloat16).astype(jnp.float32)
        charge_ref[3 * piece : 3 * piece + 3, atoms : 2 * atoms] = part
        xyz = xyz - part
    value = charge_ref[...].astype(jnp.bfloat16)

    for k in range(send_ref.shape[0]):
        send_ref[k] = value


def last_kernel(
    all_ref, xyz_ref, energy_ref, out_ref, columns_ref, wide_ref, total_ref, *,
    inner, share, states, atoms,
):
    groups, _, rows = out_ref.shape
    monomers = rows // states
    pos, group = lax.axis_index("inner"), lax.axis_index("grp")
    which = (pos * share) // states
    columns_ref[...] = jnp.transpose(
        jnp.concatenate([xyz_ref[...], jnp.zeros((5, xyz_ref.shape[1]), jnp.float32)], axis=0)
    )

    for k in range(groups):
        total = all_ref[k * inner].astype(jnp.float32)
        for i in range(1, inner):
            total = total + all_ref[k * inner + i].astype(jnp.float32)
        total_ref[k] = total
    for k in range(groups):
        pieces = all_ref[k * inner + which].astype(jnp.float32)
        wide_ref[:, k * atoms : (k + 1) * atoms] = (
            pieces[0:3, atoms:] + pieces[3:6, atoms:] + pieces[6:9, atoms:]
        )
    own = total_ref[group]
    weights = []
    for c in range(monomers):
        square = None
        for axis in range(3):
            diff = (
                columns_ref[c * atoms : (c + 1) * atoms, axis : axis + 1]
                - wide_ref[axis : axis + 1, :]
            )
            square = diff * diff if square is None else square + diff * diff
        inverse = 1.0 / jnp.sqrt(square + 1.0)
        weights.append(
            jnp.dot(
                own[c * states : (c + 1) * states, :atoms], inverse,
                precision=lax.Precision.HIGHEST, preferred_element_type=jnp.float32,
            )
        )
    weight = jnp.concatenate(weights, axis=0)
    row = lax.broadcasted_iota(jnp.int32, (share, rows), 1)
    column = pos * share + lax.broadcasted_iota(jnp.int32, (share, rows), 0)
    energy = energy_ref[0:1, :rows]
    for k in range(groups):
        block = lax.dot_general(
            total_ref[k, pl.ds(pos * share, share), :atoms],
            weight[:, k * atoms : (k + 1) * atoms], NT,
            precision=lax.Precision.HIGHEST, preferred_element_type=jnp.float32,
        )
        same = (row // states == column // states) & (group == k)
        out_ref[k] = jnp.where(same, jnp.where(row == column, energy, 0.0), block)


def local(
    amplitudes, factors, atom_charges, eps_occ, eps_vir, occ_count, vir_count, atom_list, positions
):
    monomers, states, pairs = amplitudes.shape
    aux = factors.shape[1]
    atoms = atom_charges.shape[1]
    nvir = eps_vir.shape[1]
    inner, groups = lax.axis_size("inner"), lax.axis_size("grp")
    rows = monomers * states
    share = rows // inner
    assert pairs % nvir == 0 and states % share == 0 and 2 * atoms == LANES and rows >= 9 and monomers <= inner
    f32, bf16 = jnp.float32, jnp.bfloat16

    def shift(value, axis, size, k):
        return lax.ppermute(value, axis, [(i, i ^ k) for i in range(size)])

    amplitudes = amplitudes.reshape(rows, pairs)
    amps = [shift(amplitudes, "inner", inner, r) for r in range(1, inner)]
    tiles = factors.shape[2] // LANES
    stored = factors.transpose(1, 0, 2).reshape(aux, monomers, tiles, LANES).transpose(0, 2, 1, 3)
    cuts = [*range(0, aux, CHUNK), aux]
    if cuts[-1] - cuts[-2] > CHUNK // 2:
        cuts.insert(-1, (aux - TAIL) // 8 * 8)
    chunks = [(q, end - q) for q, end in zip(cuts, cuts[1:])]
    factor_here, fit, sums, own_xyz, masked, active, inverse = pl.pallas_call(
        functools.partial(first_kernel, chunks=chunks),
        in_specs=[HBM] * 8,
        out_specs=[VMEM] * 7,
        out_shape=[
            pltpu.VMEM((tiles, aux * monomers, LANES), bf16),
            jax.ShapeDtypeStruct((rows, aux * monomers), f32),
            jax.ShapeDtypeStruct((rows, LANES), f32),
            jax.ShapeDtypeStruct((3, monomers * atoms), f32),
            jax.ShapeDtypeStruct((rows, pairs), bf16),
            jax.ShapeDtypeStruct((monomers, inner * pairs), f32),
            jax.ShapeDtypeStruct((monomers, pairs), f32),
        ],
        scratch_shapes=[
            pltpu.SMEM(occ_count.shape, jnp.int32),
            pltpu.SMEM(vir_count.shape, jnp.int32),
            pltpu.SMEM(eps_occ.shape, f32),
            pltpu.VMEM(eps_vir.shape, f32),
            pltpu.VMEM((rows, pairs), bf16),
            pltpu.VMEM((1, monomers * atoms), jnp.int32),
            pltpu.VMEM(positions.shape, f32),
            pltpu.SemaphoreType.DMA((len(chunks),)),
            pltpu.SemaphoreType.DMA((7,)),
        ],
        compiler_params=PARAMS,
        name="first",
    )(
        *[
            pltpu.with_memory_space_constraint(x, pltpu.HBM)
            for x in (
                occ_count, vir_count, eps_occ, eps_vir, amplitudes, atom_list[None, :], positions,
            )
        ],
        stored,
    )
    factor_here = pltpu.with_memory_space_constraint(factor_here, pltpu.VMEM)
    order = sorted(range(1, inner), key=lambda r: -r.bit_length()) + [0]
    part = jax.ShapeDtypeStruct((rows, pairs + LANES), bf16)
    low, pieces = pl.pallas_call(
        functools.partial(second_kernel, inner=inner, monomers=monomers),
        in_specs=[VMEM] * (inner + 3),
        out_specs=[VMEM] * 2,
        out_shape=[
            jax.ShapeDtypeStruct((rows, aux * monomers), bf16),
            jax.ShapeDtypeStruct((rows, LANES), bf16),
        ],
        scratch_shapes=[pltpu.VMEM((inner - 1, rows, pairs), bf16)],
        compiler_params=PARAMS,
        name="second",
    )(*amps, factor_here, fit, sums, active)
    got = []
    for r in order:
        block = pl.pallas_call(
            functools.partial(part_kernel, r=r),
            in_specs=[VMEM] * 3,
            out_specs=VMEM,
            out_shape=part,
            compiler_params=PARAMS,
            cost_estimate=pl.CostEstimate(flops=COST, transcendentals=0, bytes_accessed=0),
            name="part",
        )(low, pieces, factor_here)
        got.append(shift(block, "inner", inner, r) if r else block)
    refined, send, energies = pl.pallas_call(
        functools.partial(third_kernel, inner=inner),
        in_specs=[VMEM] * (inner + 4),
        out_specs=[VMEM] * 3,
        out_shape=[
            jax.ShapeDtypeStruct((rows, pairs), f32),
            jax.ShapeDtypeStruct((groups * inner, rows, LANES), bf16),
            jax.ShapeDtypeStruct((8, rows), f32),
        ],
        scratch_shapes=[
            pltpu.VMEM((rows, LANES), f32),
            pltpu.VMEM((monomers, states, pairs), bf16),
        ],
        compiler_params=PARAMS,
        name="third",
    )(masked, inverse, atom_charges, *got, own_xyz)
    everyone = lax.all_to_all(send, ("grp", "inner"), 0, 0, tiled=True)
    block = pl.pallas_call(
        functools.partial(last_kernel, inner=inner, share=share, states=states, atoms=atoms),
        in_specs=[VMEM] * 3,
        out_specs=VMEM,
        out_shape=jax.ShapeDtypeStruct((groups, share, rows), f32),
        scratch_shapes=[
            pltpu.VMEM((monomers * atoms, 8), f32),
            pltpu.VMEM((3, groups * atoms), f32),
            pltpu.VMEM((groups, rows, LANES), f32),
        ],
        compiler_params=PARAMS,
        name="last",
    )(everyone, own_xyz, energies)
    return refined.reshape(monomers, states, pairs), block.transpose(2, 0, 1)


def solution(mesh):
    in_specs = (
        P("grp", None, "inner"),
        P("grp", "inner", None),
        P("grp", None, "inner"),
        P("grp", None),
        P("grp", None),
        P("grp"),
        P("grp"),
        P("grp"),
        P(),
    )
    out_specs = (P("grp", None, "inner"), P("grp", None, "inner"))

    return jax.shard_map(local, mesh=mesh, in_specs=in_specs, out_specs=out_specs, check_vma=False)
```
